256 devices in a mesh: px: 4 (over x_lo, core), py: 8 (over y, x_hi), pz: 8 (over z).
Axes of the slice: x: 4 (x_hi: 2, x_lo: 2; x = x_hi * 2 + x_lo), y: 4, z: 8, core: 2. Of those that a mesh axis runs over, the one named last changes fastest.
Arguments:
- control_values: float32 [28, 56, 56, 512], P('px', 'py', 'pz'), may hold values from -6 to 6
- metric_diag: float32 [3, 32, 4096], P(None, 'px', ('py', 'pz')), may hold values from 0.5 to 2
- metric_off: float32 [3, 32, 4096], P(None, 'px', ('py', 'pz')), may hold values from -0.2 to 0.2
- mass_weight: float32 [32, 4096], P('px', ('py', 'pz')), may hold values from 0.5 to 2
- orient: int32 [4, 8, 8, 3], P('px', 'py', 'pz'), may hold values from 0 to 1
Outputs:
- stiffness_out: float32 [28, 56, 56, 512], P('px', 'py', 'pz')
- mass_out: float32 [28, 56, 56, 512], P('px', 'py', 'pz')
The draws below stay inside these ranges and needn't reach their ends.
All inputs are finite; a program needn't handle non-finite values.
Results may differ from the reference program's by a relative error of at most 0.0003.
Values sent between devices are 32-bit elements; how exact they have to be, the bound alone decides.
No kernel may reach another device: no remote copies, remote signals or barrier semaphores. Data moves between devices by JAX's collectives and lax.ppermute only.
A program may use at most 64 MiB of HBM per device.

```python
import math
import jax
import jax.numpy as jnp
import numpy as np
from jax import lax

ELEMS = 4
VECS = 512
CTRL = 7
QUAD = 8
N_PX = 4
N_PY = 8
N_PZ = 8


def touch_ends(drawn, own_key, smallest, top_value):
    shape = drawn.shape
    index_at = [jax.random.randint(jax.random.fold_in(own_key, axis), (), 0, shape[axis]) for axis in range(len(shape))]
    drawn = drawn.at[tuple(index_at)].set(smallest)
    longest = shape.index(max(shape))
    index_at[longest] = (index_at[longest] + 1) % shape[longest]
    return drawn.at[tuple(index_at)].set(top_value)


def levels(rng, dims, split, least, high):
    loudness = 1.0
    for axis_at, blocks in split:
        draws = jax.random.uniform(jax.random.fold_in(jax.random.fold_in(rng, 6), axis_at), (blocks,), jnp.float32, least / len(split), high / len(split))
        loudness = loudness * jnp.repeat(jnp.exp(draws), dims[axis_at] // blocks).reshape((-1,) + (1,) * (len(dims) - 1 - axis_at))
    return loudness


def bell_draw(stream_key, shape, deviation, most, split=(), held_as=jnp.bfloat16):
    result = deviation * jax.random.normal(stream_key, shape, jnp.float32)
    if split:
        result = result * levels(stream_key, shape, split, -0.22, 0.18)
    return jnp.clip(result, -most, most).astype(held_as)


def setup_inputs(seed: int = 0) -> dict:
    key_of = jax.random.split(jax.random.key(seed), 6)
    return {
        "control_values": bell_draw(key_of[0], (N_PX * CTRL, N_PY * CTRL, N_PZ * CTRL, VECS), 1.0, 6.0, ((0, 4), (1, 8), (2, 8)), jnp.float32),
        "metric_diag": jnp.clip(jnp.exp(math.log(2.0) - 1.3862944 * jax.random.uniform(key_of[1], (3, N_PX * QUAD, N_PY * N_PZ * QUAD * QUAD), jnp.float32) ** levels(key_of[1], (3, N_PX * QUAD, N_PY * N_PZ * QUAD * QUAD), ((1, 4), (2, 64)), -0.2, 0.2)), 0.5, 2.0),
        "metric_off": jnp.clip(jax.random.uniform(key_of[2], (3, N_PX * QUAD, N_PY * N_PZ * QUAD * QUAD), jnp.float32, -0.2, 0.2) * levels(key_of[2], (3, N_PX * QUAD, N_PY * N_PZ * QUAD * QUAD), ((1, 4), (2, 64)), -0.4, 0.0), -0.2, 0.2),
        "mass_weight": jnp.clip(jnp.exp(math.log(2.0) - 1.3862944 * jax.random.uniform(key_of[3], (N_PX * QUAD, N_PY * N_PZ * QUAD * QUAD), jnp.float32) ** levels(key_of[3], (N_PX * QUAD, N_PY * N_PZ * QUAD * QUAD), ((0, 4), (1, 64)), -0.2, 0.2)), 0.5, 2.0),
        "orient": touch_ends(jax.random.randint(key_of[4], (N_PX, N_PY, N_PZ, 3), 0, 2), jax.random.fold_in(key_of[4], 1), 0, 1).astype(jnp.int32),
    }


def spline_tables(elements):
    knot_row = np.concatenate([np.zeros(3), np.arange(elements + 1) * 1.0, np.full(3, float(elements))])
    offsets = np.array([0.5 - 0.5 / math.sqrt(3.0), 0.5 + 0.5 / math.sqrt(3.0)])
    points = (np.arange(elements)[:, None] + offsets[None, :]).reshape(-1)
    intervals = np.repeat(np.arange(elements), 2) + 3
    current = np.zeros((points.size, knot_row.size - 1))
    current[np.arange(points.size), intervals] = 1.0
    previous = current
    for degree in range(1, 4):
        columns = knot_row.size - 1 - degree
        updated = np.zeros((points.size, columns))
        for i in range(columns):
            lower_gap = knot_row[i + degree] - knot_row[i]
            upper_gap = knot_row[i + degree + 1] - knot_row[i + 1]
            if lower_gap > 0:
                updated[:, i] += (points - knot_row[i]) / lower_gap * current[:, i]
            if upper_gap > 0:
                updated[:, i] += (knot_row[i + degree + 1] - points) / upper_gap * current[:, i + 1]
        previous = current
        current = updated
    slopes = np.zeros(current.shape)
    for i in range(current.shape[1]):
        lower_gap = knot_row[i + 3] - knot_row[i]
        upper_gap = knot_row[i + 4] - knot_row[i + 1]
        if lower_gap > 0:
            slopes[:, i] += 3.0 / lower_gap * previous[:, i]
        if upper_gap > 0:
            slopes[:, i] -= 3.0 / upper_gap * previous[:, i + 1]
    return (current.astype(np.float32), slopes.astype(np.float32))

def contract(pattern, operand, table_part):
    return jnp.einsum(pattern, operand, table_part, precision=lax.Precision.HIGHEST)

def forward_parts(coeffs, values, slopes):
    along_b = contract('ijkv,ck->ijcv', coeffs, values)
    along_d = contract('ijkv,ck->ijcv', coeffs, slopes)
    plain = contract('ijcv,bj->ibcv', along_b, values)
    slope_y = contract('ijcv,bj->ibcv', along_b, slopes)
    slope_z = contract('ijcv,bj->ibcv', along_d, values)
    return (plain, slope_y, slope_z)

def stiffness_apply(parts, diag_terms, off_terms, values, slopes, block_rows):
    plain, slope_y, slope_z = parts
    quad_count = values.shape[0]
    back_x = jnp.zeros(plain.shape, jnp.float32)
    back_y = jnp.zeros(plain.shape, jnp.float32)
    back_z = jnp.zeros(plain.shape, jnp.float32)
    for first_row in range(0, quad_count, block_rows):
        last_row = first_row + block_rows
        slope_rows = slopes[first_row:last_row]
        value_rows = values[first_row:last_row]
        grad_x = contract('ibcv,ai->abcv', plain, slope_rows)
        grad_y = contract('ibcv,ai->abcv', slope_y, value_rows)
        grad_z = contract('ibcv,ai->abcv', slope_z, value_rows)
        diag_rows = diag_terms[:, first_row:last_row, :, :, None]
        off_rows = off_terms[:, first_row:last_row, :, :, None]
        flux_x = diag_rows[0] * grad_x + off_rows[0] * grad_y + off_rows[1] * grad_z
        flux_y = off_rows[0] * grad_x + diag_rows[1] * grad_y + off_rows[2] * grad_z
        flux_z = off_rows[1] * grad_x + off_rows[2] * grad_y + diag_rows[2] * grad_z
        back_x = back_x + contract('abcv,ai->ibcv', flux_x, slope_rows)
        back_y = back_y + contract('abcv,ai->ibcv', flux_y, value_rows)
        back_z = back_z + contract('abcv,ai->ibcv', flux_z, value_rows)
    middle_b = contract('ibcv,bj->ijcv', back_x, values) + contract('ibcv,bj->ijcv', back_y, slopes)
    middle_d = contract('ibcv,bj->ijcv', back_z, values)
    return contract('ijcv,ck->ijkv', middle_b, values) + contract('ijcv,ck->ijkv', middle_d, slopes)

def mass_apply(plain, weights, values, block_rows):
    quad_count = values.shape[0]
    back_mass = jnp.zeros(plain.shape, jnp.float32)
    for first_row in range(0, quad_count, block_rows):
        last_row = first_row + block_rows
        value_rows = values[first_row:last_row]
        point_values = contract('ibcv,ai->abcv', plain, value_rows)
        weighted = weights[first_row:last_row, :, :, None] * point_values
        back_mass = back_mass + contract('abcv,ai->ibcv', weighted, value_rows)
    middle = contract('ibcv,bj->ijcv', back_mass, values)
    return contract('ijcv,ck->ijkv', middle, values)

def flip_frame(grid_data, flip_flags, first_dim):
    for d in range(3):
        grid_data = jnp.where(flip_flags[d] == 1, jnp.flip(grid_data, axis=first_dim + d), grid_data)
    return grid_data

def fold_axis(grid_data, patch_axis, point_axis):
    extent = grid_data.shape[point_axis]
    first_plane = lax.slice_in_dim(grid_data, 0, 1, axis=point_axis)
    last_plane = lax.slice_in_dim(grid_data, extent - 1, extent, axis=point_axis)
    middle = lax.slice_in_dim(grid_data, 1, extent - 1, axis=point_axis)
    from_before = jnp.roll(last_plane, 1, axis=patch_axis)
    from_after = jnp.roll(first_plane, -1, axis=patch_axis)
    return jnp.concatenate([first_plane + from_before, middle, last_plane + from_after], axis=point_axis)

def reference(control_values, metric_diag, metric_off, mass_weight, orient):
    values_np, slopes_np = spline_tables(ELEMS)
    values = jnp.asarray(values_np)
    slopes = jnp.asarray(slopes_np)
    patches = N_PX * N_PY * N_PZ
    coeffs = control_values.reshape(N_PX, CTRL, N_PY, CTRL, N_PZ, CTRL, VECS)
    coeffs = coeffs.transpose(0, 2, 4, 1, 3, 5, 6).reshape(patches, CTRL, CTRL, CTRL, VECS)
    diag_all = metric_diag.reshape(3, N_PX, QUAD, N_PY, N_PZ, QUAD, QUAD)
    diag_all = diag_all.transpose(1, 3, 4, 0, 2, 5, 6).reshape(patches, 3, QUAD, QUAD, QUAD)
    off_all = metric_off.reshape(3, N_PX, QUAD, N_PY, N_PZ, QUAD, QUAD)
    off_all = off_all.transpose(1, 3, 4, 0, 2, 5, 6).reshape(patches, 3, QUAD, QUAD, QUAD)
    weight_all = mass_weight.reshape(N_PX, QUAD, N_PY, N_PZ, QUAD, QUAD)
    weight_all = weight_all.transpose(0, 2, 3, 1, 4, 5).reshape(patches, QUAD, QUAD, QUAD)
    flag_all = orient.reshape(patches, 3)

    def one_patch(patch_items):
        coeff_patch, diag_patch, off_patch, weight_patch, flag_patch = patch_items
        parts = forward_parts(coeff_patch, values, slopes)
        stiffness = stiffness_apply(parts, diag_patch, off_patch, values, slopes, QUAD)
        mass_part = mass_apply(parts[0], weight_patch, values, QUAD)
        return (flip_frame(stiffness, flag_patch, 0), flip_frame(mass_part, flag_patch, 0))
    stiffness_all, mass_all = lax.map(one_patch, (coeffs, diag_all, off_all, weight_all, flag_all))

    def assemble(grid_data):
        grid_data = grid_data.reshape(N_PX, N_PY, N_PZ, CTRL, CTRL, CTRL, VECS)
        grid_data = fold_axis(grid_data, 0, 3)
        grid_data = fold_axis(grid_data, 1, 4)
        grid_data = fold_axis(grid_data, 2, 5)
        return grid_data.reshape(patches, CTRL, CTRL, CTRL, VECS)

    def flip_back(patch_items):
        stiff_patch, mass_patch, flag_patch = patch_items
        return (flip_frame(stiff_patch, flag_patch, 0), flip_frame(mass_patch, flag_patch, 0))
    stiffness_all, mass_all = lax.map(flip_back, (assemble(stiffness_all), assemble(mass_all), flag_all))

    def to_layout(grid_data):
        grid_data = grid_data.reshape(N_PX, N_PY, N_PZ, CTRL, CTRL, CTRL, VECS)
        return grid_data.transpose(0, 3, 1, 4, 2, 5, 6).reshape(N_PX * CTRL, N_PY * CTRL, N_PZ * CTRL, VECS)
    return (to_layout(stiffness_all), to_layout(mass_all))
```

```python
import functools
import math

import jax
import jax.numpy as jnp
import numpy as np
from jax import lax
from jax.experimental import pallas as pl
from jax.experimental.pallas import tpu as pltpu
from jax.sharding import PartitionSpec as P

CHUNKS = 2


def spline_tables(elements):
    knot_row = np.concatenate(
        [np.zeros(3), np.arange(elements + 1) * 1.0, np.full(3, float(elements))]
    )
    offsets = np.array([0.5 - 0.5 / math.sqrt(3.0), 0.5 + 0.5 / math.sqrt(3.0)])
    points = (np.arange(elements)[:, None] + offsets[None, :]).reshape(-1)
    intervals = np.repeat(np.arange(elements), 2) + 3
    current = np.zeros((points.size, knot_row.size - 1))
    current[np.arange(points.size), intervals] = 1.0
    previous = current
    for degree in range(1, 4):
        columns = knot_row.size - 1 - degree
        updated = np.zeros((points.size, columns))
        for i in range(columns):
            lower_gap = knot_row[i + degree] - knot_row[i]
            upper_gap = knot_row[i + degree + 1] - knot_row[i + 1]
            if lower_gap > 0:
                updated[:, i] += (points - knot_row[i]) / lower_gap * current[:, i]
            if upper_gap > 0:
                updated[:, i] += (knot_row[i + degree + 1] - points) / upper_gap * current[:, i + 1]
        previous = current
        current = updated
    slopes = np.zeros(current.shape)
    for i in range(current.shape[1]):
        lower_gap = knot_row[i + 3] - knot_row[i]
        upper_gap = knot_row[i + 4] - knot_row[i + 1]
        if lower_gap > 0:
            slopes[:, i] += 3.0 / lower_gap * previous[:, i]
        if upper_gap > 0:
            slopes[:, i] -= 3.0 / upper_gap * previous[:, i + 1]
    return (current.astype(np.float32), slopes.astype(np.float32))


VALUES, SLOPES = spline_tables(4)


def split_const(table):
    high = table.astype(jnp.bfloat16)
    low = (table - high.astype(np.float64)).astype(jnp.bfloat16)
    return high, low


def plane_table(along_j, along_k):
    out = np.zeros((8, 8, 8, 8))
    out[:, :, :7, :7] = along_j.astype(np.float64)[:, None, :, None] * along_k.astype(
        np.float64
    )[None, :, None, :]
    return out.reshape(64, 64)


def forward_table():
    table = np.concatenate(
        [
            plane_table(VALUES, VALUES),
            plane_table(SLOPES, VALUES),
            plane_table(VALUES, SLOPES),
        ]
    )
    high, low = split_const(table)
    return np.concatenate([high, high, low], axis=1)


def backward_table():
    variants = []
    for flip_j in (0, 1):
        for flip_k in (0, 1):
            values_j, slopes_j = (t[:, ::-1] if flip_j else t for t in (VALUES, SLOPES))
            values_k, slopes_k = (t[:, ::-1] if flip_k else t for t in (VALUES, SLOPES))
            plain = plane_table(values_j, values_k).T
            stiff = np.concatenate(
                [plain, plane_table(slopes_j, values_k).T, plane_table(values_j, slopes_k).T, 0 * plain],
                axis=1,
            )
            mass = np.concatenate([0 * plain] * 3 + [plain], axis=1)
            rows = [stiff, mass]
            for part in (stiff, mass):
                rows += [part[0::8], part[6::8]]
            high, low = split_const(np.concatenate(rows))
            variants.append(np.concatenate([high, low], axis=1))
    return np.stack(variants)


def apply_kernel(
    flags, u, diag, off, weight, forward, backward, grid_out, x_low, x_high, y_low, y_high,
    z_low, z_high, padded, fields, fluxes, metric, staged,
):
    width = u.shape[3]

    @pl.when(pl.program_id(0) == 0)
    def _():
        padded[...] = jnp.zeros_like(padded)
        staged[...] = jnp.zeros_like(staged)
        for s in range(3):
            staged[8 * s : 8 * s + 8, 0:64] = diag[s]
            staged[24 + 8 * s : 32 + 8 * s, 0:64] = off[s]
        staged[48:56, 0:64] = weight[...]
        turned = staged[...].T
        for row in range(56):
            metric[row] = jnp.broadcast_to(turned[0:64, row : row + 1], (64, 128))

    for i in range(7):
        for j in range(7):
            padded[i, 8 * j : 8 * j + 7] = u[i, j]
        block = padded[i]
        high = block.astype(jnp.bfloat16)
        low = (block - high.astype(jnp.float32)).astype(jnp.bfloat16)
        fields[i] = jnp.dot(
            forward[...],
            jnp.concatenate([high, low, high], axis=0),
            preferred_element_type=jnp.float32,
        )

    def at_points(q2, carry):
        row = pl.multiple_of(q2 * 8, 8)
        for lane in range(width // 128):
            lanes = slice(128 * lane, 128 * lane + 128)
            taken, total = {}, {}
            for element in range(4):
                active = range(element, element + 4)
                for i in active:
                    if i not in taken:
                        taken[i] = [fields[i, pl.ds(64 * f + row, 8), lanes] for f in range(3)]
                for q1 in (2 * element, 2 * element + 1):
                    def along(table, f):
                        acc = None
                        for i in active:
                            term = taken[i][f] * np.float32(table[q1, i])
                            acc = term if acc is None else acc + term
                        return acc

                    g1, g2, g3 = along(SLOPES, 0), along(VALUES, 1), along(VALUES, 2)
                    plain = along(VALUES, 0)
                    d0, d1, d2, o0, o1, o2, w = (
                        metric[8 * c + q1, pl.ds(row, 8), :] for c in range(7)
                    )
                    parts = (
                        (SLOPES, d0 * g1 + o0 * g2 + o1 * g3),
                        (VALUES, o0 * g1 + d1 * g2 + o2 * g3),
                        (VALUES, o1 * g1 + o2 * g2 + d2 * g3),
                        (VALUES, w * plain),
                    )
                    for f, (table, flux) in enumerate(parts):
                        for i in active:
                            term = flux * np.float32(table[q1, i])
                            key = (i, f)
                            total[key] = term if key not in total else total[key] + term
                finished = (element,) if element < 3 else active
                for i in finished:
                    for f in range(4):
                        fluxes[i, pl.ds(64 * f + row, 8), lanes] = total.pop((i, f))
        return carry

    lax.fori_loop(0, 8, at_points, 0)

    flipped = flags[0] == 1
    for i in range(7):
        block = fluxes[i]
        high = block.astype(jnp.bfloat16)
        low = (block - high.astype(jnp.float32)).astype(jnp.bfloat16)
        rows = (
            jnp.dot(backward[0, :, 0:256], high, preferred_element_type=jnp.float32)
            + jnp.dot(backward[0, :, 256:512], high, preferred_element_type=jnp.float32)
            + jnp.dot(backward[0, :, 0:256], low, preferred_element_type=jnp.float32)
        )
        spot = jnp.where(flipped, 6 - i, i)
        for f in range(2):
            for j in range(7):
                first = 64 * f + 8 * j
                grid_out[f, spot, j] = rows[first : first + 7]
            y_low[f, spot] = rows[64 * f : 64 * f + 7]
            y_high[f, spot] = rows[64 * f + 48 : 64 * f + 55]
            z_low[f, spot] = rows[128 + 16 * f : 135 + 16 * f]
            z_high[f, spot] = rows[136 + 16 * f : 143 + 16 * f]
    x_low[...] = grid_out[:, 0]
    x_high[...] = grid_out[:, 6]


def apply(flags, control_values, diag, off, weight):
    width = control_values.shape[3] // CHUNKS
    forward = jnp.asarray(forward_table())
    backward = jnp.asarray(backward_table())
    plane = jax.ShapeDtypeStruct((2, 7, 7, control_values.shape[3]), jnp.float32)
    plane_spec = pl.BlockSpec((2, 7, 7, width), lambda c, flags: (0, 0, 0, c))
    whole = lambda *shape: pl.BlockSpec(shape, lambda c, flags: (0,) * len(shape))
    return pl.pallas_call(
        apply_kernel,
        out_shape=[jax.ShapeDtypeStruct((2, 7, 7, 7, control_values.shape[3]), jnp.float32)]
        + [plane] * 6,
        grid_spec=pltpu.PrefetchScalarGridSpec(
            num_scalar_prefetch=1,
            grid=(CHUNKS,),
            in_specs=[
                pl.BlockSpec((7, 7, 7, width), lambda c, flags: (0, 0, 0, c)),
                whole(3, 8, 64),
                whole(3, 8, 64),
                whole(8, 64),
                whole(192, 192),
                pl.BlockSpec((1, 160, 512), lambda c, flags: (2 * flags[1] + flags[2], 0, 0)),
            ],
            out_specs=[pl.BlockSpec((2, 7, 7, 7, width), lambda c, flags: (0, 0, 0, 0, c))]
            + [plane_spec] * 6,
            scratch_shapes=[
                pltpu.VMEM((7, 64, width), jnp.float32),
                pltpu.VMEM((7, 192, width), jnp.float32),
                pltpu.VMEM((7, 256, width), jnp.float32),
                pltpu.VMEM((56, 64, 128), jnp.float32),
                pltpu.VMEM((128, 128), jnp.float32),
            ],
        ),
        compiler_params=pltpu.CompilerParams(vmem_limit_bytes=40 * 1024 * 1024),
        name="apply",
    )(flags, control_values, diag, off, weight, forward, backward)


def lines_kernel(count, *refs):
    planes, received, outs = refs[:2], refs[2 : 2 + 2 * count], refs[2 + 2 * count :]
    from_z = received[0:2]
    for plane, out, end in zip(planes, outs, (0, 6)):
        for p in range(7):
            for f in range(2):
                low, high = (
                    r[f, end, p : p + 1] if count == 1 else r[f, p, end : end + 1] for r in from_z
                )
                block = plane[f, p]
                if count == 2 and p == 0:
                    block = block + received[2][f, end]
                if count == 2 and p == 6:
                    block = block + received[3][f, end]
                out[f, p, 0:1] = block[0:1] + low
                out[f, p, 1:6] = block[1:6]
                out[f, p, 6:7] = block[6:7] + high


def add_lines(planes, *received):
    plane = jax.ShapeDtypeStruct(planes[0].shape, jnp.float32)
    return pl.pallas_call(
        functools.partial(lines_kernel, len(received) // 2),
        out_shape=[plane, plane],
        compiler_params=pltpu.CompilerParams(vmem_limit_bytes=8 * 1024 * 1024),
        name="add_lines",
    )(*planes, *received)


def finish_kernel(flags, grid_in, x_low, x_high, y_low, y_high, z_low, z_high, stiff, mass):
    lanes = grid_in.shape[4]
    flip_i, flip_j, flip_k = (flags[d] == 1 for d in range(3))
    spots = lax.broadcasted_iota(jnp.int32, (8, lanes), 0)
    source = jnp.where(spots < 7, jnp.where(flip_k, 6 - spots, spots), spots)
    pad = jnp.zeros((1, lanes), jnp.float32)
    at_low = (spots == 0).astype(jnp.float32)
    for f, out in ((0, stiff), (1, mass)):
        for i in range(7):
            for j in range(7):
                block = grid_in[f, i, j]
                if i == 0:
                    block = block + x_low[f, j]
                if i == 6:
                    block = block + x_high[f, j]
                if j == 0:
                    block = block + y_low[f, i]
                if j == 6:
                    block = block + y_high[f, i]
                block = jnp.concatenate(
                    [
                        block[0:1] + z_low[f, i, j : j + 1],
                        block[1:6],
                        block[6:7] + z_high[f, i, j : j + 1],
                        pad,
                    ],
                    axis=0,
                )
                turned = jnp.take_along_axis(block, source, axis=0)
                out[jnp.where(flip_i, 6 - i, i), jnp.where(flip_j, 6 - j, j)] = turned[0:7]


def finish(flags, grid_data, planes):
    vecs = grid_data.shape[4]
    width = vecs // CHUNKS
    plane_spec = pl.BlockSpec((2, 7, 7, width), lambda c, flags: (0, 0, 0, c))
    out_spec = pl.BlockSpec((7, 7, 7, width), lambda c, flags: (0, 0, 0, c))
    out = jax.ShapeDtypeStruct((7, 7, 7, vecs), jnp.float32)
    return pl.pallas_call(
        finish_kernel,
        out_shape=[out, out],
        grid_spec=pltpu.PrefetchScalarGridSpec(
            num_scalar_prefetch=1,
            grid=(CHUNKS,),
            in_specs=[pl.BlockSpec((2, 7, 7, 7, width), lambda c, flags: (0, 0, 0, 0, c))]
            + [plane_spec] * 6,
            out_specs=[out_spec, out_spec],
        ),
        compiler_params=pltpu.CompilerParams(vmem_limit_bytes=40 * 1024 * 1024),
        name="finish",
    )(flags, grid_data, *planes)


def exchange(low, high, axis):
    size = lax.axis_size(axis)
    up = [(i, (i + 1) % size) for i in range(size)]
    down = [(j, i) for i, j in up]
    return lax.ppermute(high, axis, up), lax.ppermute(low, axis, down)


def per_device(control_values, metric_diag, metric_off, mass_weight, orient):
    flags = orient.reshape(3)
    grid_data, x_low, x_high, y_low, y_high, z_low, z_high = apply(
        flags, control_values, metric_diag, metric_off, mass_weight
    )
    from_z = exchange(z_low, z_high, "pz")
    from_x = exchange(*add_lines((x_low, x_high), *from_z), "px")
    from_y = exchange(*add_lines((y_low, y_high), *from_z, *from_x), "py")
    stiffness, mass = finish(flags, grid_data, from_x + from_y + from_z)
    return stiffness, mass


def solution(mesh):
    in_specs = (
        P("px", "py", "pz", None),
        P(None, "px", ("py", "pz")),
        P(None, "px", ("py", "pz")),
        P("px", ("py", "pz")),
        P("px", "py", "pz", None),
    )
    out_specs = (P("px", "py", "pz", None), P("px", "py", "pz", None))
    return jax.shard_map(
        per_device, mesh=mesh, in_specs=in_specs, out_specs=out_specs, check_vma=False
    )
```

```python
import math

import jax
import jax.numpy as jnp
import numpy as np
from jax import lax
from jax.experimental import pallas as pl
from jax.experimental.pallas import tpu as pltpu
from jax.sharding import PartitionSpec as P


def spline_tables(elements):
    knot_row = np.concatenate(
        [np.zeros(3), np.arange(elements + 1) * 1.0, np.full(3, float(elements))]
    )
    offsets = np.array([0.5 - 0.5 / math.sqrt(3.0), 0.5 + 0.5 / math.sqrt(3.0)])
    points = (np.arange(elements)[:, None] + offsets[None, :]).reshape(-1)
    intervals = np.repeat(np.arange(elements), 2) + 3
    current = np.zeros((points.size, knot_row.size - 1))
    current[np.arange(points.size), intervals] = 1.0
    previous = current
    for degree in range(1, 4):
        columns = knot_row.size - 1 - degree
        updated = np.zeros((points.size, columns))
        for i in range(columns):
            lower_gap = knot_row[i + degree] - knot_row[i]
            upper_gap = knot_row[i + degree + 1] - knot_row[i + 1]
            if lower_gap > 0:
                updated[:, i] += (points - knot_row[i]) / lower_gap * current[:, i]
            if upper_gap > 0:
                updated[:, i] += (knot_row[i + degree + 1] - points) / upper_gap * current[:, i + 1]
        previous = current
        current = updated
    slopes = np.zeros(current.shape)
    for i in range(current.shape[1]):
        lower_gap = knot_row[i + 3] - knot_row[i]
        upper_gap = knot_row[i + 4] - knot_row[i + 1]
        if lower_gap > 0:
            slopes[:, i] += 3.0 / lower_gap * previous[:, i]
        if upper_gap > 0:
            slopes[:, i] -= 3.0 / upper_gap * previous[:, i + 1]
    return (current.astype(np.float32), slopes.astype(np.float32))


VALUES, SLOPES = spline_tables(4)


def split_const(table):
    high = table.astype(jnp.bfloat16)
    low = (table - high.astype(np.float64)).astype(jnp.bfloat16)
    return high, low


def plane_table(along_j, along_k):
    out = np.zeros((8, 8, 8, 8))
    out[:, :, :7, :7] = along_j.astype(np.float64)[:, None, :, None] * along_k.astype(
        np.float64
    )[None, :, None, :]
    return out.reshape(64, 64)


def forward_table():
    table = np.concatenate(
        [
            plane_table(VALUES, VALUES),
            plane_table(SLOPES, VALUES),
            plane_table(VALUES, SLOPES),
        ]
    )
    high, low = split_const(table)
    return np.concatenate([high, high, low], axis=1)


def backward_table():
    variants = []
    for flip_j in (0, 1):
        for flip_k in (0, 1):
            values_j, slopes_j = (t[:, ::-1] if flip_j else t for t in (VALUES, SLOPES))
            values_k, slopes_k = (t[:, ::-1] if flip_k else t for t in (VALUES, SLOPES))
            plain = plane_table(values_j, values_k).T
            stiff = np.concatenate(
                [plain, plane_table(slopes_j, values_k).T, plane_table(values_j, slopes_k).T, 0 * plain],
                axis=1,
            )
            mass = np.concatenate([0 * plain] * 3 + [plain], axis=1)
            rows = [stiff, mass]
            for part in (stiff, mass):
                rows += [part[0::8], part[6::8]]
            high, low = split_const(np.concatenate(rows))
            variants.append(np.concatenate([high, low], axis=1))
    return np.stack(variants)


def accumulate(fields, metric, row, lanes, elements, sums):
    taken = {}
    for element in elements:
        active = range(element, element + 4)
        for i in active:
            if i not in taken:
                taken[i] = [fields[i, pl.ds(64 * f + row, 8), lanes] for f in range(3)]
        for q1 in (2 * element, 2 * element + 1):
            def along(table, f):
                acc = None
                for i in active:
                    term = taken[i][f] * np.float32(table[q1, i])
                    acc = term if acc is None else acc + term
                return acc

            g1, g2, g3 = along(SLOPES, 0), along(VALUES, 1), along(VALUES, 2)
            plain = along(VALUES, 0)
            d0, d1, d2, o0, o1, o2, w = (metric[8 * c + q1, pl.ds(row, 8), :] for c in range(7))
            parts = (
                (SLOPES, d0 * g1 + o0 * g2 + o1 * g3),
                (VALUES, o0 * g1 + d1 * g2 + o2 * g3),
                (VALUES, o1 * g1 + o2 * g2 + d2 * g3),
                (VALUES, w * plain),
            )
            for f, (table, flux) in enumerate(parts):
                for i in active:
                    term = flux * np.float32(table[q1, i])
                    sums[i][f] = term if sums[i][f] is None else sums[i][f] + term


def spread_metric(turned, metric, rows_of_q1):
    for c in range(7):
        for q1 in rows_of_q1:
            row = 8 * c + q1
            metric[row] = jnp.broadcast_to(turned[0:64, row : row + 1], (64, 128))


def backward_rows(table, fluxes):
    high = fluxes.astype(jnp.bfloat16)
    low = (fluxes - high.astype(jnp.float32)).astype(jnp.bfloat16)
    return (
        jnp.dot(table[:, 0:256], high, preferred_element_type=jnp.float32)
        + jnp.dot(table[:, 256:512], high, preferred_element_type=jnp.float32)
        + jnp.dot(table[:, 0:256], low, preferred_element_type=jnp.float32)
    )


OUTER, INNER = (0, 3), (1, 2)


def outer_kernel(
    u, diag, off, weight, orient, forward, backward, x_low, x_high, z_ends, fields, fluxes,
    turned, table, u_in, padded, metric, staged, small, forward_in, flags, sems,
):
    vecs = u.shape[3]
    copies = [
        pltpu.make_async_copy(orient, flags, sems.at[0]),
        pltpu.make_async_copy(diag, small.at[0:3], sems.at[1]),
        pltpu.make_async_copy(off, small.at[3:6], sems.at[2]),
        pltpu.make_async_copy(weight, small.at[6], sems.at[3]),
        pltpu.make_async_copy(forward, forward_in, sems.at[4]),
    ]
    loads = [pltpu.make_async_copy(u.at[i], u_in.at[i], sems.at[6 + i]) for i in range(7)]
    for copy in copies + loads:
        copy.start()
    padded[...] = jnp.zeros_like(padded)
    staged[...] = jnp.zeros_like(staged)
    copies[0].wait()
    flip_i, flip_j, flip_k = (flags[0, 0, 0, d] for d in range(3))
    copies.append(
        pltpu.make_async_copy(backward.at[2 * flip_j + flip_k], table, sems.at[5])
    )
    copies[5].start()
    for n in (1, 2, 3):
        copies[n].wait()
    for c in range(7):
        staged[8 * c : 8 * c + 8, 0:64] = small[c]
    turned[...] = staged[...].T
    spread_metric(turned, metric, (0, 1, 6, 7))
    copies[4].wait()

    for i in range(7):
        loads[i].wait()
        for j in range(7):
            padded[i, 8 * j : 8 * j + 7] = u_in[i, j]
        block = padded[i]
        high = block.astype(jnp.bfloat16)
        low = (block - high.astype(jnp.float32)).astype(jnp.bfloat16)
        fields[i] = jnp.dot(
            forward_in[...],
            jnp.concatenate([high, low, high], axis=0),
            preferred_element_type=jnp.float32,
        )

    def at_points(q2, carry):
        row = pl.multiple_of(q2 * 8, 8)
        for lane in range(vecs // 128):
            lanes = slice(128 * lane, 128 * lane + 128)
            sums = [[None] * 4 for _ in range(7)]
            accumulate(fields, metric, row, lanes, OUTER, sums)
            for i in range(7):
                for f in range(4):
                    fluxes[i, pl.ds(64 * f + row, 8), lanes] = sums[i][f]
        return carry

    lax.fori_loop(0, 8, at_points, 0)

    copies[5].wait()
    for side, out in enumerate((x_low, x_high)):
        rows = backward_rows(table, fluxes[jnp.where(flip_i == 1, 6 - 6 * side, 6 * side)])
        for f in range(2):
            for j in range(7):
                out[f, j] = rows[64 * f + 8 * j : 64 * f + 8 * j + 7]
        z_ends[side] = rows[128:160]


def inner_kernel(flags, fields, partial, turned, table, grid_out, z_inner, metric, fluxes):
    vecs = fields.shape[2]
    spread_metric(turned, metric, (2, 3, 4, 5))

    def at_points(q2, carry):
        row = pl.multiple_of(q2 * 8, 8)
        for lane in range(vecs // 128):
            lanes = slice(128 * lane, 128 * lane + 128)
            sums = [[None] * 4 for _ in range(7)]
            for i in range(1, 6):
                sums[i] = [partial[i, pl.ds(64 * f + row, 8), lanes] for f in range(4)]
            accumulate(fields, metric, row, lanes, INNER, sums)
            for i in range(1, 6):
                for f in range(4):
                    fluxes[i - 1, pl.ds(64 * f + row, 8), lanes] = sums[i][f]
        return carry

    lax.fori_loop(0, 8, at_points, 0)

    for spot in range(1, 6):
        rows = backward_rows(table, fluxes[jnp.where(flags[0] == 1, 6 - spot, spot) - 1])
        for f in range(2):
            for j in range(7):
                grid_out[f, spot - 1, j] = rows[64 * f + 8 * j : 64 * f + 8 * j + 7]
        z_inner[spot - 1] = rows[128:160]


def apply_outer(control_values, diag, off, weight, orient):
    vecs = control_values.shape[3]
    plane = jax.ShapeDtypeStruct((2, 7, 7, vecs), jnp.float32)
    shapes = [
        plane,
        plane,
        jax.ShapeDtypeStruct((2, 32, vecs), jnp.float32),
        jax.ShapeDtypeStruct((7, 192, vecs), jnp.float32),
        jax.ShapeDtypeStruct((7, 256, vecs), jnp.float32),
        jax.ShapeDtypeStruct((128, 128), jnp.float32),
        jax.ShapeDtypeStruct((160, 512), jnp.bfloat16),
    ]
    return pl.pallas_call(
        outer_kernel,
        out_shape=shapes,
        in_specs=[pl.BlockSpec(memory_space=pltpu.HBM)] * 7,
        scratch_shapes=[
            pltpu.VMEM((7, 7, 7, vecs), jnp.float32),
            pltpu.VMEM((7, 64, vecs), jnp.float32),
            pltpu.VMEM((56, 64, 128), jnp.float32),
            pltpu.VMEM((128, 128), jnp.float32),
            pltpu.VMEM((7, 8, 64), jnp.float32),
            pltpu.VMEM((192, 192), jnp.bfloat16),
            pltpu.SMEM((1, 1, 1, 3), jnp.int32),
            pltpu.SemaphoreType.DMA((13,)),
        ],
        compiler_params=pltpu.CompilerParams(vmem_limit_bytes=24 * 1024 * 1024),
        cost_estimate=pl.CostEstimate(flops=400_000_000, bytes_accessed=1_000_000, transcendentals=0),
        name="apply_outer",
    )(
        *(
            pltpu.with_memory_space_constraint(x, pltpu.HBM)
            for x in (
                control_values, diag, off, weight, orient,
                jnp.asarray(forward_table()), jnp.asarray(backward_table()),
            )
        )
    )


def apply_inner(flags, fields, fluxes, turned, table):
    vecs = fields.shape[2]
    return pl.pallas_call(
        inner_kernel,
        out_shape=[
            jax.ShapeDtypeStruct((2, 5, 7, 7, vecs), jnp.float32),
            jax.ShapeDtypeStruct((5, 32, vecs), jnp.float32),
        ],
        in_specs=[pl.BlockSpec(memory_space=pltpu.SMEM)] + [pl.BlockSpec(memory_space=pltpu.VMEM)] * 4,
        scratch_shapes=[
            pltpu.VMEM((56, 64, 128), jnp.float32),
            pltpu.VMEM((5, 256, vecs), jnp.float32),
        ],
        compiler_params=pltpu.CompilerParams(vmem_limit_bytes=20 * 1024 * 1024),
        cost_estimate=pl.CostEstimate(flops=400_000_000, bytes_accessed=1_000_000, transcendentals=0),
        name="apply_inner",
    )(flags, fields, fluxes, turned, table)


def small_call(kernel, shapes, *arrays, name):
    return pl.pallas_call(
        kernel,
        out_shape=shapes,
        compiler_params=pltpu.CompilerParams(vmem_limit_bytes=4 * 1024 * 1024),
        name=name,
    )(*arrays)


def planes_kernel(x_low, x_high, from_low, from_high, grid, z_ends, z_inner, y_low, y_high, z_low, z_high):
    for f in range(2):
        for end, y_out, z_out in ((0, y_low, z_low), (6, y_high, z_high)):
            group = 8 * (2 * f + (end == 6))
            for i in range(1, 6):
                y_out[f, i] = grid[f, i - 1, end]
                z_out[f, i] = z_inner[i - 1, group : group + 7]
            for side, (own, other) in enumerate(((x_low, from_low), (x_high, from_high))):
                y_out[f, 6 * side] = own[f, end] + other[f, end]
                for j in range(7):
                    z_out[f, 6 * side, j : j + 1] = (
                        z_ends[side, group + j : group + j + 1] + other[f, j, end : end + 1]
                    )


def lines_kernel(y_low, y_high, z_low, z_high):
    for end, out in ((0, z_low), (6, z_high)):
        for f in range(2):
            for side, plane in enumerate((y_low, y_high)):
                for i in range(7):
                    out[f, side, i : i + 1] = plane[f, i, end : end + 1]


def turn_source(flip_k, lanes):
    spots = lax.broadcasted_iota(jnp.int32, (8, lanes), 0)
    return jnp.where(spots < 7, jnp.where(flip_k, 6 - spots, spots), spots)


def own_block(f, i, j, grid, x_low, x_high, from_low, from_high):
    if i == 0:
        return x_low[f, j] + from_low[f, j]
    if i == 6:
        return x_high[f, j] + from_high[f, j]
    return grid[f, i - 1, j]


def turn_block(block, low_row, high_row, source):
    pad = jnp.zeros_like(low_row)
    block = jnp.concatenate([block[0:1] + low_row, block[1:6], block[6:7] + high_row, pad], axis=0)
    return jnp.take_along_axis(block, source, axis=0)[0:7]


def finish_inner_kernel(
    flags, grid, x_low, x_high, from_low, from_high, z_low, z_high, stiff, mass, ready, sems
):
    flip_i, flip_j, flip_k = (flags[d] == 1 for d in range(3))
    source = turn_source(flip_k, grid.shape[4])
    for f, out in ((0, stiff), (1, mass)):
        for i in range(7):
            for j in range(1, 6):
                block = own_block(f, i, j, grid, x_low, x_high, from_low, from_high)
                block = turn_block(block, z_low[f, i, j : j + 1], z_high[f, i, j : j + 1], source)
                ready[f, jnp.where(flip_i, 6 - i, i), jnp.where(flip_j, 6 - j, j) - 1] = block
        pltpu.make_async_copy(ready.at[f], out.at[:, 1:6], sems.at[f]).start()
    for f, out in ((0, stiff), (1, mass)):
        pltpu.make_async_copy(ready.at[f], out.at[:, 1:6], sems.at[f]).wait()


def finish_outer_kernel(
    flags, stiff_in, mass_in, grid, x_low, x_high, from_low, from_high, y_low, y_high, z_low,
    z_high, line_low, line_high, stiff, mass, ready, sems,
):
    flip_i, flip_j, flip_k = (flags[d] == 1 for d in range(3))
    source = turn_source(flip_k, grid.shape[4])
    copies = []
    for f, out in ((0, stiff), (1, mass)):
        for i in range(7):
            for side, plane in enumerate((y_low, y_high)):
                j = 6 * side
                block = own_block(f, i, j, grid, x_low, x_high, from_low, from_high) + plane[f, i]
                block = turn_block(
                    block,
                    z_low[f, i, j : j + 1] + line_low[f, side, i : i + 1],
                    z_high[f, i, j : j + 1] + line_high[f, side, i : i + 1],
                    source,
                )
                ready[f, jnp.where(flip_j, 1 - side, side), jnp.where(flip_i, 6 - i, i)] = block
        for side in range(2):
            copy = pltpu.make_async_copy(ready.at[f, side], out.at[:, 6 * side], sems.at[2 * f + side])
            copy.start()
            copies.append(copy)
    for copy in copies:
        copy.wait()


def exchange(low, high, axis):
    size = lax.axis_size(axis)
    up = [(i, (i + 1) % size) for i in range(size)]
    down = [(j, i) for i, j in up]
    return lax.ppermute(high, axis, up), lax.ppermute(low, axis, down)


def per_device(control_values, metric_diag, metric_off, mass_weight, orient):
    vecs = control_values.shape[3]
    flags = orient.reshape(3)
    out = jax.ShapeDtypeStruct((7, 7, 7, vecs), jnp.float32)
    plane = jax.ShapeDtypeStruct((2, 7, 7, vecs), jnp.float32)
    in_smem, in_vmem, in_hbm = (pl.BlockSpec(memory_space=m) for m in (pltpu.SMEM, pltpu.VMEM, pltpu.HBM))
    x_low, x_high, z_ends, fields, fluxes, turned, table = apply_outer(
        control_values, metric_diag, metric_off, mass_weight, orient
    )
    from_x = exchange(x_low, x_high, "px")
    grid, z_inner = apply_inner(flags, fields, fluxes, turned, table)
    own = (grid, x_low, x_high) + from_x
    y_low, y_high, z_low, z_high = small_call(
        planes_kernel, [plane] * 4, x_low, x_high, *from_x, grid, z_ends, z_inner, name="planes"
    )
    from_y = exchange(y_low, y_high, "py")
    from_z = exchange(z_low, z_high, "pz")
    done = pl.pallas_call(
        finish_inner_kernel,
        out_shape=[out, out],
        in_specs=[in_smem] + [in_vmem] * 7,
        out_specs=[in_hbm, in_hbm],
        scratch_shapes=[pltpu.VMEM((2, 7, 5, 7, vecs), jnp.float32), pltpu.SemaphoreType.DMA((2,))],
        compiler_params=pltpu.CompilerParams(vmem_limit_bytes=8 * 1024 * 1024),
        cost_estimate=pl.CostEstimate(flops=100_000_000, bytes_accessed=1_000_000, transcendentals=0),
        name="finish_inner",
    )(flags, *own, *from_z)
    line = jax.ShapeDtypeStruct((2, 2, 7, vecs), jnp.float32)
    from_lines = exchange(*small_call(lines_kernel, [line] * 2, *from_y, name="lines"), "pz")
    stiffness, mass = pl.pallas_call(
        finish_outer_kernel,
        out_shape=[out, out],
        in_specs=[in_smem, in_hbm, in_hbm] + [in_vmem] * 11,
        out_specs=[in_hbm, in_hbm],
        input_output_aliases={1: 0, 2: 1},
        scratch_shapes=[pltpu.VMEM((2, 2, 7, 7, vecs), jnp.float32), pltpu.SemaphoreType.DMA((4,))],
        compiler_params=pltpu.CompilerParams(vmem_limit_bytes=8 * 1024 * 1024),
        name="finish_outer",
    )(flags, *done, *own, *from_y, *from_z, *from_lines)
    return stiffness, mass


def solution(mesh):
    in_specs = (
        P("px", "py", "pz", None),
        P(None, "px", ("py", "pz")),
        P(None, "px", ("py", "pz")),
        P("px", ("py", "pz")),
        P("px", "py", "pz", None),
    )
    out_specs = (P("px", "py", "pz", None), P("px", "py", "pz", None))
    return jax.shard_map(
        per_device, mesh=mesh, in_specs=in_specs, out_specs=out_specs, check_vma=False
    )
```

```python
import math

import jax
import jax.numpy as jnp
import numpy as np
from jax import lax
from jax.experimental import pallas as pl
from jax.experimental.pallas import tpu as pltpu
from jax.sharding import PartitionSpec as P


def spline_tables(elements):
    knot_row = np.concatenate(
        [np.zeros(3), np.arange(elements + 1) * 1.0, np.full(3, float(elements))]
    )
    offsets = np.array([0.5 - 0.5 / math.sqrt(3.0), 0.5 + 0.5 / math.sqrt(3.0)])
    points = (np.arange(elements)[:, None] + offsets[None, :]).reshape(-1)
    intervals = np.repeat(np.arange(elements), 2) + 3
    current = np.zeros((points.size, knot_row.size - 1))
    current[np.arange(points.size), intervals] = 1.0
    previous = current
    for degree in range(1, 4):
        columns = knot_row.size - 1 - degree
        updated = np.zeros((points.size, columns))
        for i in range(columns):
            lower_gap = knot_row[i + degree] - knot_row[i]
            upper_gap = knot_row[i + degree + 1] - knot_row[i + 1]
            if lower_gap > 0:
                updated[:, i] += (points - knot_row[i]) / lower_gap * current[:, i]
            if upper_gap > 0:
                updated[:, i] += (knot_row[i + degree + 1] - points) / upper_gap * current[:, i + 1]
        previous = current
        current = updated
    slopes = np.zeros(current.shape)
    for i in range(current.shape[1]):
        lower_gap = knot_row[i + 3] - knot_row[i]
        upper_gap = knot_row[i + 4] - knot_row[i + 1]
        if lower_gap > 0:
            slopes[:, i] += 3.0 / lower_gap * previous[:, i]
        if upper_gap > 0:
            slopes[:, i] -= 3.0 / upper_gap * previous[:, i + 1]
    return (current.astype(np.float32), slopes.astype(np.float32))


VALUES, SLOPES = spline_tables(4)


def split_const(table):
    high = table.astype(jnp.bfloat16)
    low = (table - high.astype(np.float64)).astype(jnp.bfloat16)
    return high, low


def plane_table(along_j, along_k):
    out = np.zeros((8, 8, 8, 8))
    out[:, :, :7, :7] = along_j.astype(np.float64)[:, None, :, None] * along_k.astype(
        np.float64
    )[None, :, None, :]
    return out.reshape(64, 64)


def forward_table():
    table = np.concatenate(
        [
            plane_table(VALUES, VALUES),
            plane_table(SLOPES, VALUES),
            plane_table(VALUES, SLOPES),
        ]
    )
    high, low = split_const(table)
    return np.concatenate([high, high, low], axis=1)


def backward_table():
    variants = []
    for flip_j in (0, 1):
        for flip_k in (0, 1):
            values_j, slopes_j = (t[:, ::-1] if flip_j else t for t in (VALUES, SLOPES))
            values_k, slopes_k = (t[:, ::-1] if flip_k else t for t in (VALUES, SLOPES))
            plain = plane_table(values_j, values_k).T
            stiff = np.concatenate(
                [plain, plane_table(slopes_j, values_k).T, plane_table(values_j, slopes_k).T, 0 * plain],
                axis=1,
            )
            mass = np.concatenate([0 * plain] * 3 + [plain], axis=1)
            rows = [stiff, mass]
            for part in (stiff, mass):
                rows += [part[0::8], part[6::8]]
            high, low = split_const(np.concatenate(rows))
            variants.append(np.concatenate([high, low], axis=1))
    return np.stack(variants)


def accumulate(fields, metric, row, lanes, elements, wanted, sums):
    taken = {}
    for element in elements:
        active = range(element, element + 4)
        for i in active:
            if i not in taken:
                taken[i] = [fields[i, pl.ds(64 * f + row, 8), lanes] for f in range(3)]
        for q1 in (2 * element, 2 * element + 1):
            def along(table, f):
                acc = None
                for i in active:
                    term = taken[i][f] * np.float32(table[q1, i])
                    acc = term if acc is None else acc + term
                return acc

            g1, g2, g3 = along(SLOPES, 0), along(VALUES, 1), along(VALUES, 2)
            plain = along(VALUES, 0)
            d0, d1, d2, o0, o1, o2, w = (metric[8 * c + q1, pl.ds(row, 8), :] for c in range(7))
            parts = (
                (SLOPES, d0 * g1 + o0 * g2 + o1 * g3),
                (VALUES, o0 * g1 + d1 * g2 + o2 * g3),
                (VALUES, o1 * g1 + o2 * g2 + d2 * g3),
                (VALUES, w * plain),
            )
            for f, (table, flux) in enumerate(parts):
                for i in wanted:
                    if i not in active:
                        continue
                    term = flux * np.float32(table[q1, i])
                    sums[i][f] = term if sums[i][f] is None else sums[i][f] + term


def spread_metric(turned, metric, rows_of_q1):
    for c in range(7):
        for q1 in rows_of_q1:
            row = 8 * c + q1
            metric[row] = jnp.broadcast_to(turned[0:64, row : row + 1], (64, 128))


def backward_rows(table, fluxes):
    high = fluxes.astype(jnp.bfloat16)
    low = (fluxes - high.astype(jnp.float32)).astype(jnp.bfloat16)
    return (
        jnp.dot(table[:, 0:256], high, preferred_element_type=jnp.float32)
        + jnp.dot(table[:, 256:512], high, preferred_element_type=jnp.float32)
        + jnp.dot(table[:, 0:256], low, preferred_element_type=jnp.float32)
    )


def put(message, f, a, block):
    count = block.shape[1] // 128
    for lane in range(count):
        message[pl.ds(count * 7 * (7 * f + a) + lane, 7, stride=count), :] = block[
            :, 128 * lane : 128 * lane + 128
        ]


def get(message, f, a):
    count = message.shape[0] // 98
    first = count * 7 * (7 * f + a)
    return jnp.concatenate(
        [message[pl.ds(first + lane, 7, stride=count), :] for lane in range(count)], axis=1
    )


def get_row(message, f, a, b):
    count = message.shape[0] // 98
    first = count * (7 * (7 * f + a) + b)
    return jnp.concatenate(
        [message[first + lane : first + lane + 1, :] for lane in range(count)], axis=1
    )


def outer_kernel(
    u, diag, off, weight, orient, forward, backward, x_low, x_high, send_low, send_high, z_ends,
    fields, turned, table, u_in, padded, fluxes, metric, staged, small, forward_in, flags, sems,
):
    vecs = u.shape[3]
    copies = [
        pltpu.make_async_copy(orient, flags, sems.at[0]),
        pltpu.make_async_copy(diag, small.at[0:3], sems.at[1]),
        pltpu.make_async_copy(off, small.at[3:6], sems.at[2]),
        pltpu.make_async_copy(weight, small.at[6], sems.at[3]),
        pltpu.make_async_copy(forward, forward_in, sems.at[4]),
    ]
    loads = [pltpu.make_async_copy(u.at[i], u_in.at[i], sems.at[6 + i]) for i in range(7)]
    for copy in copies + loads:
        copy.start()
    padded[...] = jnp.zeros_like(padded)
    staged[...] = jnp.zeros_like(staged)
    copies[0].wait()
    flip_i, flip_j, flip_k = (flags[0, 0, 0, d] for d in range(3))
    copies.append(
        pltpu.make_async_copy(backward.at[2 * flip_j + flip_k], table, sems.at[5])
    )
    copies[5].start()
    for n in (1, 2, 3):
        copies[n].wait()
    for c in range(7):
        staged[8 * c : 8 * c + 8, 0:64] = small[c]
    turned[...] = staged[...].T
    spread_metric(turned, metric, (0, 1, 6, 7))
    for copy in copies[4:5] + loads:
        copy.wait()

    for i in range(7):
        for j in range(7):
            padded[i, 8 * j : 8 * j + 7] = u_in[i, j]
        block = padded[i]
        high = block.astype(jnp.bfloat16)
        low = (block - high.astype(jnp.float32)).astype(jnp.bfloat16)
        fields[i] = jnp.dot(
            forward_in[...],
            jnp.concatenate([high, low, high], axis=0),
            preferred_element_type=jnp.float32,
        )

    def at_points(q2, carry):
        row = pl.multiple_of(q2 * 8, 8)
        for lane in range(vecs // 128):
            lanes = slice(128 * lane, 128 * lane + 128)
            sums = [[None] * 4 for _ in range(7)]
            accumulate(fields, metric, row, lanes, (0, 3), (0, 6), sums)
            for side in range(2):
                for f in range(4):
                    fluxes[side, pl.ds(64 * f + row, 8), lanes] = sums[6 * side][f]
        return carry

    lax.fori_loop(0, 8, at_points, 0)

    copies[5].wait()
    for side, (out, message) in enumerate(((x_low, send_low), (x_high, send_high))):
        rows = backward_rows(table, fluxes[jnp.where(flip_i == 1, 1 - side, side)])
        for f in range(2):
            for j in range(7):
                block = rows[64 * f + 8 * j : 64 * f + 8 * j + 7]
                out[f, j] = block
                put(message, f, j, block)
        z_ends[side] = rows[128:160]


def inner_kernel(
    orient, fields, turned, table, grid_out, z_inner, metric, fluxes, flags, sem
):
    vecs = fields.shape[2]
    fetch = pltpu.make_async_copy(orient, flags, sem)
    fetch.start()
    spread_metric(turned, metric, range(8))

    def at_points(q2, carry):
        row = pl.multiple_of(q2 * 8, 8)
        for lane in range(vecs // 128):
            lanes = slice(128 * lane, 128 * lane + 128)
            sums = [[None] * 4 for _ in range(7)]
            accumulate(fields, metric, row, lanes, range(4), range(1, 6), sums)
            for i in range(1, 6):
                for f in range(4):
                    fluxes[i - 1, pl.ds(64 * f + row, 8), lanes] = sums[i][f]
        return carry

    lax.fori_loop(0, 8, at_points, 0)

    fetch.wait()
    flipped = flags[0, 0, 0, 0] == 1
    for spot in range(1, 6):
        rows = backward_rows(table, fluxes[jnp.where(flipped, 6 - spot, spot) - 1])
        for f in range(2):
            for j in range(7):
                grid_out[f, spot - 1, j] = rows[64 * f + 8 * j : 64 * f + 8 * j + 7]
        z_inner[spot - 1] = rows[128:160]


def apply_outer(control_values, diag, off, weight, orient):
    vecs = control_values.shape[3]
    plane = jax.ShapeDtypeStruct((2, 7, 7, vecs), jnp.float32)
    message = jax.ShapeDtypeStruct((98 * vecs // 128, 128), jnp.float32)
    shapes = [
        plane,
        plane,
        message,
        message,
        jax.ShapeDtypeStruct((2, 32, vecs), jnp.float32),
        jax.ShapeDtypeStruct((7, 192, vecs), jnp.float32),
        jax.ShapeDtypeStruct((128, 128), jnp.float32),
        jax.ShapeDtypeStruct((160, 512), jnp.bfloat16),
    ]
    return pl.pallas_call(
        outer_kernel,
        out_shape=shapes,
        in_specs=[pl.BlockSpec(memory_space=pltpu.HBM)] * 7,
        scratch_shapes=[
            pltpu.VMEM((7, 7, 7, vecs), jnp.float32),
            pltpu.VMEM((7, 64, vecs), jnp.float32),
            pltpu.VMEM((2, 256, vecs), jnp.float32),
            pltpu.VMEM((56, 64, 128), jnp.float32),
            pltpu.VMEM((128, 128), jnp.float32),
            pltpu.VMEM((7, 8, 64), jnp.float32),
            pltpu.VMEM((192, 192), jnp.bfloat16),
            pltpu.SMEM((1, 1, 1, 3), jnp.int32),
            pltpu.SemaphoreType.DMA((13,)),
        ],
        compiler_params=pltpu.CompilerParams(vmem_limit_bytes=24 * 1024 * 1024),
        cost_estimate=pl.CostEstimate(flops=400_000_000, bytes_accessed=1_000_000, transcendentals=0),
        name="apply_outer",
    )(
        *(
            pltpu.with_memory_space_constraint(x, pltpu.HBM)
            for x in (
                control_values, diag, off, weight, orient,
                jnp.asarray(forward_table()), jnp.asarray(backward_table()),
            )
        )
    )


def apply_inner(orient, fields, turned, table):
    vecs = fields.shape[2]
    return pl.pallas_call(
        inner_kernel,
        out_shape=[
            jax.ShapeDtypeStruct((2, 5, 7, 7, vecs), jnp.float32),
            jax.ShapeDtypeStruct((5, 32, vecs), jnp.float32),
        ],
        in_specs=[pl.BlockSpec(memory_space=pltpu.HBM)] + [pl.BlockSpec(memory_space=pltpu.VMEM)] * 3,
        scratch_shapes=[
            pltpu.VMEM((56, 64, 128), jnp.float32),
            pltpu.VMEM((5, 256, vecs), jnp.float32),
            pltpu.SMEM((1, 1, 1, 3), jnp.int32),
            pltpu.SemaphoreType.DMA,
        ],
        compiler_params=pltpu.CompilerParams(vmem_limit_bytes=20 * 1024 * 1024),
        cost_estimate=pl.CostEstimate(flops=400_000_000, bytes_accessed=1_000_000, transcendentals=0),
        name="apply_inner",
    )(pltpu.with_memory_space_constraint(orient, pltpu.HBM), fields, turned, table)


def small_call(kernel, shapes, *arrays, name):
    return pl.pallas_call(
        kernel,
        out_shape=shapes,
        compiler_params=pltpu.CompilerParams(vmem_limit_bytes=4 * 1024 * 1024),
        name=name,
    )(*arrays)


def planes_kernel(x_low, x_high, from_low, from_high, grid, z_ends, z_inner, y_low, y_high, z_low, z_high):
    for f in range(2):
        for end, y_out, z_out in ((0, y_low, z_low), (6, y_high, z_high)):
            group = 8 * (2 * f + (end == 6))
            for i in range(1, 6):
                put(y_out, f, i, grid[f, i - 1, end])
                z_out[f, i] = z_inner[i - 1, group : group + 7]
            for side, (own, other) in enumerate(((x_low, from_low), (x_high, from_high))):
                put(y_out, f, 6 * side, own[f, end] + get(other, f, end))
                for j in range(7):
                    z_out[f, 6 * side, j : j + 1] = (
                        z_ends[side, group + j : group + j + 1] + get_row(other, f, j, end)
                    )


def lines_kernel(y_low, y_high, z_low, z_high):
    for end, out in ((0, z_low), (6, z_high)):
        for f in range(2):
            for side, plane in enumerate((y_low, y_high)):
                for i in range(7):
                    out[f, side, i : i + 1] = get_row(plane, f, i, end)


def turn_source(flip_k, lanes):
    spots = lax.broadcasted_iota(jnp.int32, (8, lanes), 0)
    return jnp.where(spots < 7, jnp.where(flip_k, 6 - spots, spots), spots)


def own_block(f, i, j, grid, x_low, x_high, from_low, from_high):
    if i == 0:
        return x_low[f, j] + get(from_low, f, j)
    if i == 6:
        return x_high[f, j] + get(from_high, f, j)
    return grid[f, i - 1, j]


def turn_block(block, low_row, high_row, source):
    pad = jnp.zeros_like(low_row)
    block = jnp.concatenate([block[0:1] + low_row, block[1:6], block[6:7] + high_row, pad], axis=0)
    return jnp.take_along_axis(block, source, axis=0)[0:7]


def finish_inner_kernel(
    flags, grid, x_low, x_high, from_low, from_high, z_low, z_high, stiff, mass, ready, sems
):
    flip_i, flip_j, flip_k = (flags[d] == 1 for d in range(3))
    source = turn_source(flip_k, grid.shape[4])
    for f, out in ((0, stiff), (1, mass)):
        for i in range(7):
            for j in range(1, 6):
                block = own_block(f, i, j, grid, x_low, x_high, from_low, from_high)
                block = turn_block(block, z_low[f, i, j : j + 1], z_high[f, i, j : j + 1], source)
                ready[f, jnp.where(flip_i, 6 - i, i), jnp.where(flip_j, 6 - j, j) - 1] = block
        pltpu.make_async_copy(ready.at[f], out.at[:, 1:6], sems.at[f]).start()
    for f, out in ((0, stiff), (1, mass)):
        pltpu.make_async_copy(ready.at[f], out.at[:, 1:6], sems.at[f]).wait()


def finish_outer_kernel(
    flags, stiff_in, mass_in, grid, x_low, x_high, from_low, from_high, y_low, y_high, z_low,
    z_high, line_low, line_high, stiff, mass, ready, sems,
):
    flip_i, flip_j, flip_k = (flags[d] == 1 for d in range(3))
    source = turn_source(flip_k, grid.shape[4])
    copies = []
    for f, out in ((0, stiff), (1, mass)):
        for i in range(7):
            for side, plane in enumerate((y_low, y_high)):
                j = 6 * side
                block = own_block(f, i, j, grid, x_low, x_high, from_low, from_high)
                block = block + get(plane, f, i)
                block = turn_block(
                    block,
                    z_low[f, i, j : j + 1] + line_low[f, side, i : i + 1],
                    z_high[f, i, j : j + 1] + line_high[f, side, i : i + 1],
                    source,
                )
                ready[f, jnp.where(flip_j, 1 - side, side), jnp.where(flip_i, 6 - i, i)] = block
        for side in range(2):
            copy = pltpu.make_async_copy(ready.at[f, side], out.at[:, 6 * side], sems.at[2 * f + side])
            copy.start()
            copies.append(copy)
    for copy in copies:
        copy.wait()


def exchange(low, high, axis):
    size = lax.axis_size(axis)
    up = [(i, (i + 1) % size) for i in range(size)]
    down = [(j, i) for i, j in up]
    return lax.ppermute(high, axis, up), lax.ppermute(low, axis, down)


def per_device(control_values, metric_diag, metric_off, mass_weight, orient):
    vecs = control_values.shape[3]
    flags = orient.reshape(3)
    out = jax.ShapeDtypeStruct((7, 7, 7, vecs), jnp.float32)
    plane = jax.ShapeDtypeStruct((2, 7, 7, vecs), jnp.float32)
    message = jax.ShapeDtypeStruct((98 * vecs // 128, 128), jnp.float32)
    in_smem, in_vmem, in_hbm = (pl.BlockSpec(memory_space=m) for m in (pltpu.SMEM, pltpu.VMEM, pltpu.HBM))
    x_low, x_high, send_low, send_high, z_ends, fields, turned, table = apply_outer(
        control_values, metric_diag, metric_off, mass_weight, orient
    )
    from_x = exchange(send_low, send_high, "px")
    grid, z_inner = apply_inner(orient, fields, turned, table)
    own = (grid, x_low, x_high) + from_x
    y_low, y_high, z_low, z_high = small_call(
        planes_kernel, [message] * 2 + [plane] * 2, x_low, x_high, *from_x, grid, z_ends, z_inner, name="planes"
    )
    from_y = exchange(y_low, y_high, "py")
    from_z = exchange(z_low, z_high, "pz")
    done = pl.pallas_call(
        finish_inner_kernel,
        out_shape=[out, out],
        in_specs=[in_smem] + [in_vmem] * 7,
        out_specs=[in_hbm, in_hbm],
        scratch_shapes=[pltpu.VMEM((2, 7, 5, 7, vecs), jnp.float32), pltpu.SemaphoreType.DMA((2,))],
        compiler_params=pltpu.CompilerParams(vmem_limit_bytes=8 * 1024 * 1024),
        cost_estimate=pl.CostEstimate(flops=100_000_000, bytes_accessed=1_000_000, transcendentals=0),
        name="finish_inner",
    )(flags, *own, *from_z)
    line = jax.ShapeDtypeStruct((2, 2, 7, vecs), jnp.float32)
    from_lines = exchange(*small_call(lines_kernel, [line] * 2, *from_y, name="lines"), "pz")
    stiffness, mass = pl.pallas_call(
        finish_outer_kernel,
        out_shape=[out, out],
        in_specs=[in_smem, in_hbm, in_hbm] + [in_vmem] * 11,
        out_specs=[in_hbm, in_hbm],
        input_output_aliases={1: 0, 2: 1},
        scratch_shapes=[pltpu.VMEM((2, 2, 7, 7, vecs), jnp.float32), pltpu.SemaphoreType.DMA((4,))],
        compiler_params=pltpu.CompilerParams(vmem_limit_bytes=8 * 1024 * 1024),
        name="finish_outer",
    )(flags, *done, *own, *from_y, *from_z, *from_lines)
    return stiffness, mass


def solution(mesh):
    in_specs = (
        P("px", "py", "pz", None),
        P(None, "px", ("py", "pz")),
        P(None, "px", ("py", "pz")),
        P("px", ("py", "pz")),
        P("px", "py", "pz", None),
    )
    out_specs = (P("px", "py", "pz", None), P("px", "py", "pz", None))
    return jax.shard_map(
        per_device, mesh=mesh, in_specs=in_specs, out_specs=out_specs, check_vma=False
    )
```
